32 devices in a mesh: dp: 8 (over z, x), tensor: 4 (over y, core).
Axes of the slice: x: 2, y: 2, z: 4, core: 2. Of those that a mesh axis runs over, the one named last changes fastest.
Arguments:
- ranges: bfloat16 [10240, 2652], P('dp'), may hold values from 0.049804688 to 2
- pot: float32 [10240], P('dp'), may hold values from 0.1 to 1
- w_ranges: bfloat16 [2652, 2048], P(None, 'tensor'), may hold values from -0.125 to 0.125
- w_pot: float32 [2048], P('tensor'), may hold values from -5 to 5
- bias_one: float32 [2048], P('tensor'), may hold values from -1.5 to 1.5
- w_two: bfloat16 [2048, 2048], P('dp', 'tensor'), may hold values from -0.125 to 0.125
- bias_two: float32 [2048], P('tensor'), may hold values from -1.5 to 1.5
- w_three: bfloat16 [2048, 2048], P('dp', 'tensor'), may hold values from -0.125 to 0.125
- bias_three: float32 [2048], P('tensor'), may hold values from -1.5 to 1.5
- w_out: bfloat16 [2048, 2652], P(('dp', 'tensor')), may hold values from -0.1875 to 0.1875
- bias_out: float32 [2652], replicated, may hold values from -1.5 to 1.5
Outputs:
- hand_values: float32 [10240, 2652], P(('dp', 'tensor'))
The draws below stay inside these ranges and needn't reach their ends.
All inputs are finite; a program needn't handle non-finite values.
Results may differ from the reference program's by a relative error of at most 0.0039.
Values may be sent and summed in bfloat16 or wider, within the bound.
A program may use at most 128 MiB of HBM per device.

```python
import math
import jax
import jax.numpy as jnp

HANDS = 1326
HID = 2048
STATES = 10240


def spiked(values, own_key, source, target, blocks, factor):
    def block_of(axis_at):
        return (jnp.arange(values.shape[axis_at]) // (values.shape[axis_at] // blocks)).reshape((-1,) + (1,) * (values.ndim - 1 - axis_at))

    near = jax.random.permutation(own_key, blocks)[block_of(target)]
    far = (block_of(target) + blocks // 2) % blocks
    return jnp.where((block_of(source) == near) | (block_of(source) == far), factor * values, values)


def block_scale(stream_key, shape, cuts, least, top_value):
    level = 1.0
    for dim, shards_of in cuts:
        steps = jax.random.uniform(jax.random.fold_in(jax.random.fold_in(stream_key, 6), dim), (shards_of,), jnp.float32, least / len(cuts), top_value / len(cuts))
        level = level * jnp.repeat(jnp.exp(steps), shape[dim] // shards_of).reshape((-1,) + (1,) * (len(shape) - 1 - dim))
    return level


def gaussian(rng, extent, deviation, bound, split=(), held_as=jnp.bfloat16):
    loudness = block_scale(rng, extent, split, -0.22, 0.18) if split else 1.0
    array = jax.random.normal(rng, extent, jnp.float32) * deviation * loudness
    return jnp.minimum(jnp.maximum(array, -bound), bound).astype(held_as)


def heavy_noise(rng, extent, spread, reach, pieces, heavy, dtype=jnp.bfloat16):
    drawn = spread * jax.random.normal(rng, extent, jnp.float32)
    if pieces:
        drawn = drawn * block_scale(rng, extent, pieces, -0.22, 0.18)
    return jnp.clip(spiked(drawn, jax.random.fold_in(rng, 3), *heavy), -reach, reach).astype(dtype)


def setup_inputs(seed: int = 0) -> dict:
    key_list = jax.random.split(jax.random.key(seed), 12)
    return {
        "ranges": jnp.clip(jnp.exp(math.log(2.0) - 3.6927934 * jax.random.uniform(key_list[0], (STATES, 2 * HANDS), jnp.float32) ** block_scale(key_list[0], (STATES, 2 * HANDS), ((0, 8),), -0.2, 0.2)), 0.049804688, 2.0).astype(jnp.bfloat16),
        "pot": jnp.clip(jnp.exp(math.log(1.0) - 2.3025851 * jax.random.uniform(key_list[1], (STATES,), jnp.float32) ** block_scale(key_list[1], (STATES,), ((0, 8),), -0.2, 0.2)), 0.1, 1.0),
        "w_ranges": gaussian(key_list[2], (2 * HANDS, HID), (2 * HANDS) ** -0.5, 0.125, ((1, 4),)),
        "w_pot": gaussian(key_list[3], (HID,), 1.0, 5.0, ((0, 4),), jnp.float32),
        "bias_one": gaussian(key_list[4], (HID,), 0.3, 1.5, ((0, 4),), jnp.float32),
        "w_two": gaussian(key_list[5], (HID, HID), HID ** -0.5, 0.125, ((0, 8), (1, 4))),
        "bias_two": gaussian(key_list[6], (HID,), 0.3, 1.5, ((0, 4),), jnp.float32),
        "w_three": gaussian(key_list[7], (HID, HID), HID ** -0.5, 0.125, ((0, 8), (1, 4))),
        "bias_three": gaussian(key_list[8], (HID,), 0.3, 1.5, ((0, 4),), jnp.float32),
        "w_out": heavy_noise(key_list[9], (HID, 2 * HANDS), HID ** -0.5, 0.1875, ((0, 32),), (0, 1, 4, 2.0)),
        "bias_out": gaussian(key_list[10], (2 * HANDS,), 0.3, 1.5, (), jnp.float32),
    }


def reference(ranges, pot, w_ranges, w_pot, bias_one, w_two, bias_two, w_three, bias_three, w_out, bias_out):
    pre = jnp.dot(ranges, w_ranges, preferred_element_type=jnp.float32)
    pre = pre + pot[:, None] * w_pot[None, :] + bias_one[None, :]
    first = jnp.maximum(pre, 0.0).astype(jnp.bfloat16)
    second = jnp.maximum(jnp.dot(first, w_two, preferred_element_type=jnp.float32) + bias_two[None, :], 0.0).astype(jnp.bfloat16)
    third = jnp.maximum(jnp.dot(second, w_three, preferred_element_type=jnp.float32) + bias_three[None, :], 0.0).astype(jnp.bfloat16)
    values = jnp.dot(third, w_out, preferred_element_type=jnp.float32) + bias_out[None, :]
    weights = ranges.astype(jnp.float32)
    error = jnp.sum(weights * values, axis=1) / jnp.sum(weights, axis=1)
    return values - error[:, None]
```

```python
import functools

import jax
import jax.numpy as jnp
from jax import lax
from jax.experimental import pallas as pl
from jax.experimental.pallas import tpu as pltpu
from jax.sharding import PartitionSpec as P

MESH = pl.DeviceIdType.MESH
CORES = 2


def relu_round(pre):
    return jnp.maximum(pre, 0.0).astype(jnp.bfloat16)


def fold_rows(left, piece):
    return jnp.dot(left, piece, preferred_element_type=jnp.float32)


def factors(dp, tensor):
    nx = max(f for f in range(1, dp + 1) if dp % f == 0 and f * f <= dp)
    return dp // nx, nx, tensor // CORES


def out_orders():
    return (("y", "z", "x"), ("y", "x", "z"))


def out_blocks(sizes):
    blocks = []
    for color, order in enumerate(out_orders()):
        for dy in range(sizes["y"]):
            for dz in range(sizes["z"]):
                for dx in range(sizes["x"]):
                    if color == 0:
                        when = 34 + 14 * dz + 8 * dx + dy
                    else:
                        when = 34 + 22 * dz + dy if dz else 17 + 12 * dx + dy
                    blocks.append((when, color, {"y": dy, "z": dz, "x": dx}))
    return sorted(blocks, key=lambda b: b[0])


def onward(order, sizes, far):
    axes = []
    for at, axis in enumerate(order):
        later = order[at + 1 :]
        if far[axis] < sizes[axis] - 1 and all(far[a] == 0 for a in later):
            axes.append(axis)
    return axes


def kernel(
    sizes, h_ref, w2_ref, w3_ref, wo_ref, b2_ref, b3_ref, third_ref, full_ref,
    act2, act3, stage2, stage3, w2_buf, w3_buf,
    w_send, w_recv, a_send, a_recv, p_recv, t_send, t_recv, o_send, o_recv, q_recv, own_sem,
):
    nz, nx, ny = sizes["z"], sizes["x"], sizes["y"]
    groups = ny * CORES
    dp_at, t_at = lax.axis_index("dp"), lax.axis_index("tensor")
    at = {
        "z": lax.div(dp_at, nx), "x": lax.rem(dp_at, nx),
        "y": lax.div(t_at, CORES), "c": lax.rem(t_at, CORES),
    }

    def shifted(axis, by):
        return lax.rem(at[axis] + by + sizes[axis], sizes[axis])

    def dev(z=None, x=None, y=None, c=None):
        z = at["z"] if z is None else z
        x = at["x"] if x is None else x
        y = at["y"] if y is None else y
        c = at["c"] if c is None else c
        return {"dp": z * nx + x, "tensor": y * CORES + c}

    nexts = {axis: dev(**{axis: shifted(axis, 1)}) for axis in ("z", "x", "y")}
    partner = dev(c=1 - at["c"])

    barrier = pltpu.get_barrier_semaphore()
    greeted = 0
    for axis in ("z", "x"):
        for by in {1 % sizes[axis], sizes[axis] - 1} - {0}:
            pl.semaphore_signal(
                barrier, inc=1, device_id=dev(**{axis: shifted(axis, by)}), device_id_type=MESH
            )
            greeted += 1
    for by in range(1, groups):
        pl.semaphore_signal(
            barrier, inc=1,
            device_id={"dp": dp_at, "tensor": lax.rem(t_at + by, groups)}, device_id_type=MESH,
        )
        greeted += 1
    pl.semaphore_wait(barrier, greeted)

    started = []

    def send(src, dst, s_sem, r_sem, to):
        copy = pltpu.make_async_remote_copy(
            src_ref=src, dst_ref=dst, send_sem=s_sem, recv_sem=r_sem,
            device_id=to, device_id_type=MESH,
        )
        copy.start()
        started.append(copy)

    def arrived(ref, sem, spare):
        pltpu.make_async_remote_copy(
            src_ref=ref, dst_ref=ref, send_sem=spare, recv_sem=sem,
            device_id=partner, device_id_type=MESH,
        ).wait_recv()

    def local_copy(src, dst, sem):
        copy = pltpu.make_async_copy(src, dst, sem)
        copy.start()
        return copy

    chunks, own, width = h_ref.shape
    depth = w2_ref.shape[0]
    sizes_w = {"z": nz, "x": nx}

    def columns(dy, core):
        piece = shifted("y", -dy) * CORES + core
        return pl.ds(pl.multiple_of(piece * width, width), width)

    def hidden_send(layer, j, dy, src):
        act = (act2, act3)[layer]
        spot = act.at[j, :, columns(dy, at["c"])]
        src = spot if src is None else src
        if dy < ny - 1:
            send(src, spot, a_send.at[layer, j, dy, 0], a_recv.at[layer, j, dy + 1], nexts["y"])
        send(src, spot, a_send.at[layer, j, dy, 1], p_recv.at[layer, j, dy], partner)

    def hidden_on(layer, j, dy):
        act = (act2, act3)[layer]
        arrived(act.at[j, :, columns(dy, at["c"])], a_recv.at[layer, j, dy], own_sem.at[0])
        hidden_send(layer, j, dy, None)

    def weight_rows(dz, dx):
        row = shifted("z", -dz) * nx + shifted("x", -dx)
        return pl.ds(pl.multiple_of(row * depth, depth), depth)

    def weight_on(layer, dz, dx):
        buf, ref = ((w2_buf, w2_ref), (w3_buf, w3_ref))[layer]
        spot = buf.at[weight_rows(dz, dx), :]
        src = spot
        if dz == 0 and dx == 0:
            src = ref
        else:
            arrived(spot, w_recv.at[layer, dz, dx], own_sem.at[0])
        for axis in onward(("z", "x"), sizes_w, {"z": dz, "x": dx}):
            to_z, to_x = (dz + 1, dx) if axis == "z" else (dz, dx + 1)
            which = 0 if axis == "z" else 1
            send(src, spot, w_send.at[layer, dz, dx, which], w_recv.at[layer, to_z, to_x], nexts[axis])

    def out_spot(color, far, core):
        row = shifted("z", -far["z"]) * nx + shifted("x", -far["x"])
        return full_ref.at[(row * groups + shifted("y", -far["y"]) * CORES + core) * 2 + color]

    def out_on(color, far, axes, wait, mate):
        order = out_orders()[color]
        spot = out_spot(color, far, at["c"])
        where = (color, far["y"], far["z"], far["x"])
        src = wo_ref.at[color] if sum(far.values()) == 0 else spot
        if wait and sum(far.values()):
            arrived(spot, o_recv.at[where], own_sem.at[0])
        for axis in onward(order, sizes, far):
            if axis not in axes:
                continue
            to = dict(far)
            to[axis] += 1
            send(
                src, spot, o_send.at[where + ("yzx".index(axis),)],
                o_recv.at[color, to["y"], to["z"], to["x"]], nexts[axis],
            )
        if mate:
            send(src, spot, o_send.at[where + (3,)], q_recv.at[where], partner)

    def compute(layer, j):
        act, buf, bias = ((act2, w2_buf, b2_ref), (act3, w3_buf, b3_ref))[layer]
        return relu_round(fold_rows(act[j], buf[...]) + bias[...])

    def pieces_here(layer, j):
        act = (act2, act3)[layer]
        for dy in range(ny):
            arrived(act.at[j, :, columns(dy, 1 - at["c"])], p_recv.at[layer, j, dy], own_sem.at[0])

    def layer_two(j):
        pieces_here(0, j)
        hidden = compute(0, j)
        stage2[j] = hidden
        act3[j, :, columns(0, at["c"])] = hidden
        hidden_send(1, j, 0, stage2.at[j])

    finals = []

    def layer_three(j):
        pieces_here(1, j)
        stage3[j] = compute(1, j)
        mine = third_ref.at[:, pl.ds(pl.multiple_of(t_at * width, width), width)]
        far = lax.rem(j - t_at + groups, groups)

        def away():
            return pltpu.make_async_remote_copy(
                src_ref=stage3.at[j], dst_ref=mine, send_sem=t_send.at[j], recv_sem=t_recv.at[far],
                device_id={"dp": dp_at, "tensor": jnp.int32(j)}, device_id_type=MESH,
            )

        def here():
            return pltpu.make_async_copy(stage3.at[j], mine, t_send.at[j])

        @pl.when(t_at != j)
        def _():
            away().start()

        @pl.when(t_at == j)
        def _():
            here().start()

        def finish():
            @pl.when(t_at != j)
            def _():
                away().wait_send()

            @pl.when(t_at == j)
            def _():
                here().wait()

        finals.append(finish)

    zero = {"y": 0, "z": 0, "x": 0}
    tasks = []
    for j in range(chunks):
        for dy in range(1, ny):
            tasks.append((9.0 * (j + 1) + 7 * (dy - 1), functools.partial(hidden_on, 0, j, dy)))
            tasks.append((36 + 7.0 * (j + 1) + 7 * (dy - 1), functools.partial(hidden_on, 1, j, dy)))
        last = 7 * (ny - 2)
        tasks.append((max(26, 9.0 * (j + 1) + last) + 0.1, functools.partial(layer_two, j)))
        tasks.append((36 + 7.0 * (j + 1) + last + 0.1, functools.partial(layer_three, j)))
    for layer, base in ((0, 0.0), (1, 17.0)):
        for dz in range(nz):
            for dx in range(nx):
                if dz + dx:
                    when = base + 5.6 * dz + (25 * layer + 25.9 if dx == nx - 1 else 6.0 * dx)
                    when = min(when, 25.95 if layer == 0 else 42.0)
                    tasks.append((when, functools.partial(weight_on, layer, dz, dx)))
    tasks.append((17.0, functools.partial(weight_on, 1, 0, 0)))
    for when, color, far in out_blocks(sizes):
        if sum(far.values()) == 0:
            tasks.append((16.5 if color else 33.0, functools.partial(out_on, color, far, "zx", False, False)))
        else:
            tasks.append((when, functools.partial(out_on, color, far, "yzx", True, True)))

    own_hidden = [
        local_copy(h_ref.at[j], act2.at[j, :, columns(0, at["c"])], own_sem.at[1 + j])
        for j in range(chunks)
    ]
    weight_on(0, 0, 0)
    for j in range(chunks):
        hidden_send(0, j, 0, h_ref.at[j])
        if j == 0:
            for color in range(2):
                out_on(color, zero, "y", False, True)
    own_out = [
        local_copy(wo_ref.at[color], out_spot(color, zero, at["c"]), own_sem.at[1 + chunks + color])
        for color in range(2)
    ]
    w2_buf[weight_rows(0, 0), :] = w2_ref[...]
    w3_buf[weight_rows(0, 0), :] = w3_ref[...]
    for copy in own_hidden:
        copy.wait()
    for _, task in sorted(tasks, key=lambda t: t[0]):
        task()

    for _, color, far in out_blocks(sizes):
        arrived(
            out_spot(color, far, 1 - at["c"]),
            q_recv.at[color, far["y"], far["z"], far["x"]], own_sem.at[0],
        )
    for by in range(1, groups):
        source = lax.rem(t_at - by + groups, groups)
        spot = third_ref.at[:, pl.ds(pl.multiple_of(source * width, width), width)]
        arrived(spot, t_recv.at[by], own_sem.at[0])
    for copy in own_out:
        copy.wait()
    for finish in finals:
        finish()
    for copy in started:
        copy.wait_send()


def middle(hidden, w_two, bias_two, w_three, bias_three, w_out):
    dp, groups = lax.axis_size("dp"), lax.axis_size("tensor")
    nz, nx, ny = factors(dp, groups)
    sizes = {"z": nz, "x": nx, "y": ny}
    states, width = hidden.shape
    own = states // groups
    rows, hands = w_out.shape
    units = width * groups
    vmem, anywhere = pl.BlockSpec(memory_space=pltpu.VMEM), pl.BlockSpec(memory_space=pl.ANY)
    dma = pltpu.SemaphoreType.DMA
    third, full = pl.pallas_call(
        functools.partial(kernel, sizes),
        out_shape=(
            jax.ShapeDtypeStruct((own, units), jnp.bfloat16),
            jax.ShapeDtypeStruct((dp * groups * 2, rows // 2, hands), jnp.bfloat16),
        ),
        in_specs=[anywhere, vmem, vmem, vmem, vmem, vmem],
        out_specs=(anywhere, anywhere),
        scratch_shapes=[
            pltpu.VMEM((groups, own, units), jnp.bfloat16),
            pltpu.VMEM((groups, own, units), jnp.bfloat16),
            pltpu.VMEM((groups, own, width), jnp.bfloat16),
            pltpu.VMEM((groups, own, width), jnp.bfloat16),
            pltpu.VMEM((units, width), jnp.bfloat16),
            pltpu.VMEM((units, width), jnp.bfloat16),
            dma((2, nz, nx, 2)),
            dma((2, nz, nx)),
            dma((2, groups, ny, 2)),
            dma((2, groups, ny)),
            dma((2, groups, ny)),
            dma((groups,)),
            dma((groups,)),
            dma((2, ny, nz, nx, 4)),
            dma((2, ny, nz, nx)),
            dma((2, ny, nz, nx)),
            dma((1 + groups + 2,)),
        ],
        compiler_params=pltpu.CompilerParams(
            collective_id=0, has_side_effects=True, vmem_limit_bytes=48 * 1024 * 1024
        ),
    )(
        hidden.reshape(groups, own, width), w_two, w_three, w_out.reshape(2, rows // 2, hands),
        bias_two[None, :], bias_three[None, :],
    )
    return third, full.reshape(units, hands)


def local(
    ranges, pot, w_ranges, w_pot, bias_one, w_two, bias_two, w_three, bias_three, w_out, bias_out
):
    groups = lax.axis_size("tensor")
    position = lax.axis_index("tensor")
    states = ranges.shape[0]
    own_count = states // groups
    lowest = position * own_count
    own_ranges = lax.dynamic_slice_in_dim(ranges, lowest, own_count, 0)
    pre = jnp.dot(ranges, w_ranges, preferred_element_type=jnp.float32)
    hidden = relu_round(pre + pot[:, None] * w_pot[None, :] + bias_one[None, :])
    own_hidden, out_whole = middle(hidden, w_two, bias_two, w_three, bias_three, w_out)
    values = fold_rows(own_hidden, out_whole) + bias_out[None, :]
    weights = own_ranges.astype(jnp.float32)
    error = jnp.sum(weights * values, axis=1) / jnp.sum(weights, axis=1)
    return values - error[:, None]


def solution(mesh):
    in_specs = (
        P("dp", None),
        P("dp"),
        P(None, "tensor"),
        P("tensor"),
        P("tensor"),
        P("dp", "tensor"),
        P("tensor"),
        P("dp", "tensor"),
        P("tensor"),
        P(("dp", "tensor"), None),
        P(),
    )
    out_specs = P(("dp", "tensor"), None)
    return jax.shard_map(local, mesh=mesh, in_specs=in_specs, out_specs=out_specs, check_vma=False)
```

```python
import functools
import math

import jax
import jax.numpy as jnp
from jax import lax
from jax.experimental import pallas as pl
from jax.experimental.pallas import tpu as pltpu
from jax.sharding import PartitionSpec as P

MESH = pl.DeviceIdType.MESH
CORES = 2
STEP = 256
W_ORDERS = (("z", "x"), ("x", "z"))


def relu_round(pre):
    return jnp.maximum(pre, 0.0).astype(jnp.bfloat16)


def fold_rows(left, piece):
    return jnp.dot(left, piece, preferred_element_type=jnp.float32)


def factors(dp, tensor):
    nx = max(f for f in range(1, dp + 1) if dp % f == 0 and f * f <= dp)
    return dp // nx, nx, tensor // CORES


def out_orders():
    return (("y", "z", "x"), ("y", "z", "x"))


def out_blocks(sizes):
    blocks = []
    for color, order in enumerate(out_orders()):
        for dy in range(sizes["y"]):
            for dz in range(sizes["z"]):
                for dx in range(sizes["x"]):
                    when = 20 + 18 * dz + 10 * color + 8 * dx + dy
                    blocks.append((when, color, {"y": dy, "z": dz, "x": dx}))
    return sorted(blocks, key=lambda b: b[0])


def onward(order, sizes, far):
    axes = []
    for at, axis in enumerate(order):
        later = order[at + 1 :]
        if far[axis] < sizes[axis] - 1 and all(far[a] == 0 for a in later):
            axes.append(axis)
    return axes


def kernel(
    sizes, ranges_ref, wr_ref, pot_ref, wp_ref, b1_ref, w2_ref, w3_ref, wo_ref, b2_ref, b3_ref,
    third_ref, full_ref, picked_ref,
    ranges_buf, wr_buf, stage1, act2, act3, stage2, stage3, w2_buf, w3_buf,
    w_send, w_recv, a_send, a_recv, p_recv, t_send, t_recv, o_send, o_recv, q_recv, own_sem,
):
    nz, nx, ny = sizes["z"], sizes["x"], sizes["y"]
    groups = ny * CORES
    dp_at, t_at = lax.axis_index("dp"), lax.axis_index("tensor")
    at = {
        "z": lax.div(dp_at, nx), "x": lax.rem(dp_at, nx),
        "y": lax.div(t_at, CORES), "c": lax.rem(t_at, CORES),
    }

    def shifted(axis, by):
        return lax.rem(at[axis] + by + sizes[axis], sizes[axis])

    def dev(z=None, x=None, y=None, c=None):
        z = at["z"] if z is None else z
        x = at["x"] if x is None else x
        y = at["y"] if y is None else y
        c = at["c"] if c is None else c
        return {"dp": z * nx + x, "tensor": y * CORES + c}

    nexts = {axis: dev(**{axis: shifted(axis, 1)}) for axis in ("z", "x", "y")}
    partner = dev(c=1 - at["c"])

    states = ranges_ref.shape[1]
    steps = states // math.gcd(states, STEP)
    tall = states // steps
    loads = [
        pltpu.make_async_copy(
            ranges_ref.at[:, pl.ds(i * tall, tall)], ranges_buf.at[:, pl.ds(i * tall, tall)],
            own_sem.at[3 + i],
        )
        for i in range(steps)
    ]
    load_wr = pltpu.make_async_copy(wr_ref, wr_buf, own_sem.at[3 + steps])
    load_wr.start()
    for load in loads:
        load.start()

    barrier = pltpu.get_barrier_semaphore()
    greeted = 0
    for axis in ("z", "x"):
        for by in {1 % sizes[axis], sizes[axis] - 1} - {0}:
            pl.semaphore_signal(
                barrier, inc=1, device_id=dev(**{axis: shifted(axis, by)}), device_id_type=MESH
            )
            greeted += 1
    for by in range(1, groups):
        pl.semaphore_signal(
            barrier, inc=1,
            device_id={"dp": dp_at, "tensor": lax.rem(t_at + by, groups)}, device_id_type=MESH,
        )
        greeted += 1
    pl.semaphore_wait(barrier, greeted)

    started = []

    def send(src, dst, s_sem, r_sem, to):
        copy = pltpu.make_async_remote_copy(
            src_ref=src, dst_ref=dst, send_sem=s_sem, recv_sem=r_sem,
            device_id=to, device_id_type=MESH,
        )
        copy.start()
        started.append(copy)

    def arrived(ref, sem, spare):
        pltpu.make_async_remote_copy(
            src_ref=ref, dst_ref=ref, send_sem=spare, recv_sem=sem,
            device_id=partner, device_id_type=MESH,
        ).wait_recv()

    def local_copy(src, dst, sem):
        copy = pltpu.make_async_copy(src, dst, sem)
        copy.start()
        return copy

    chunks, own, width = stage2.shape
    depth = w2_ref.shape[0]
    sizes_w = {"z": nz, "x": nx}

    def columns(dy, core):
        piece = shifted("y", -dy) * CORES + core
        return pl.ds(pl.multiple_of(piece * width, width), width)

    def hidden_send(layer, j, dy, src):
        act = (act2, act3)[layer]
        spot = act.at[j, :, columns(dy, at["c"])]
        src = spot if src is None else src
        if dy < ny - 1:
            send(src, spot, a_send.at[layer, j, dy, 0], a_recv.at[layer, j, dy + 1], nexts["y"])
        send(src, spot, a_send.at[layer, j, dy, 1], p_recv.at[layer, j, dy], partner)

    def hidden_on(layer, j, dy):
        act = (act2, act3)[layer]
        arrived(act.at[j, :, columns(dy, at["c"])], a_recv.at[layer, j, dy], own_sem.at[0])
        hidden_send(layer, j, dy, None)

    def weight_rows(dz, dx):
        row = shifted("z", -dz) * nx + shifted("x", -dx)
        return pl.ds(pl.multiple_of(row * depth, depth), depth)

    def weight_on(layer, dz, dx):
        buf, ref = ((w2_buf, w2_ref), (w3_buf, w3_ref))[layer]
        spot = buf.at[weight_rows(dz, dx), :]
        src = spot
        if dz == 0 and dx == 0:
            src = ref
        else:
            arrived(spot, w_recv.at[layer, dz, dx], own_sem.at[0])
        for axis in onward(W_ORDERS[layer], sizes_w, {"z": dz, "x": dx}):
            to_z, to_x = (dz + 1, dx) if axis == "z" else (dz, dx + 1)
            which = 0 if axis == "z" else 1
            send(src, spot, w_send.at[layer, dz, dx, which], w_recv.at[layer, to_z, to_x], nexts[axis])

    def out_spot(color, far, core):
        row = shifted("z", -far["z"]) * nx + shifted("x", -far["x"])
        return full_ref.at[(row * groups + shifted("y", -far["y"]) * CORES + core) * 2 + color]

    def out_on(color, far, axes, wait, mate):
        order = out_orders()[color]
        spot = out_spot(color, far, at["c"])
        where = (color, far["y"], far["z"], far["x"])
        src = wo_ref.at[color] if sum(far.values()) == 0 else spot
        if wait and sum(far.values()):
            arrived(spot, o_recv.at[where], own_sem.at[0])
        for axis in onward(order, sizes, far):
            if axis not in axes:
                continue
            to = dict(far)
            to[axis] += 1
            send(
                src, spot, o_send.at[where + ("yzx".index(axis),)],
                o_recv.at[color, to["y"], to["z"], to["x"]], nexts[axis],
            )
        if mate:
            send(src, spot, o_send.at[where + (3,)], q_recv.at[where], partner)

    def compute(layer, j):
        act, buf, bias = ((act2, w2_buf, b2_ref), (act3, w3_buf, b3_ref))[layer]
        return relu_round(fold_rows(act[j], buf[...]) + bias[...])

    def pieces_here(layer, j):
        act = (act2, act3)[layer]
        for dy in range(ny):
            arrived(act.at[j, :, columns(dy, 1 - at["c"])], p_recv.at[layer, j, dy], own_sem.at[0])

    def layer_two(j):
        pieces_here(0, j)
        hidden = compute(0, j)
        stage2[j] = hidden
        act3[j, :, columns(0, at["c"])] = hidden
        hidden_send(1, j, 0, stage2.at[j])

    def layer_one(i):
        if i == 0:
            load_wr.wait()
        loads[i].wait()
        at_rows = pl.ds(i * tall, tall)
        pre = lax.dot_general(
            ranges_buf[:, at_rows], wr_buf[...], (((0,), (0,)), ((), ())),
            preferred_element_type=jnp.float32,
        )
        stage1[at_rows, :] = relu_round(pre + pot_ref[at_rows, :] * wp_ref[...] + b1_ref[...])
        for j in range(chunks):
            if i * tall < (j + 1) * own <= (i + 1) * tall:
                rows = pl.ds(j * own, own)
                act2[j, :, columns(0, at["c"])] = stage1[rows, :]
                hidden_send(0, j, 0, stage1.at[rows, :])

    def pick():
        wanted = lax.broadcasted_iota(jnp.int32, (own, states), 0) + t_at * own
        found = lax.broadcasted_iota(jnp.int32, (own, states), 1) == wanted
        picked_ref[...] = lax.dot_general(
            jnp.where(found, 1.0, 0.0).astype(jnp.bfloat16), ranges_buf[...],
            (((1,), (1,)), ((), ())), preferred_element_type=jnp.float32,
        ).astype(jnp.bfloat16)

    finals = []

    def layer_three(j):
        pieces_here(1, j)
        stage3[j] = compute(1, j)
        mine = third_ref.at[:, pl.ds(pl.multiple_of(t_at * width, width), width)]
        far = lax.rem(j - t_at + groups, groups)

        def away():
            return pltpu.make_async_remote_copy(
                src_ref=stage3.at[j], dst_ref=mine, send_sem=t_send.at[j], recv_sem=t_recv.at[far],
                device_id={"dp": dp_at, "tensor": jnp.int32(j)}, device_id_type=MESH,
            )

        def here():
            return pltpu.make_async_copy(stage3.at[j], mine, t_send.at[j])

        @pl.when(t_at != j)
        def _():
            away().start()

        @pl.when(t_at == j)
        def _():
            here().start()

        def finish():
            @pl.when(t_at != j)
            def _():
                away().wait_send()

            @pl.when(t_at == j)
            def _():
                here().wait()

        finals.append(finish)

    zero = {"y": 0, "z": 0, "x": 0}
    tasks = []
    last = 7 * (ny - 2)
    for i in range(steps):
        tasks.append((2.0 * i, functools.partial(layer_one, i)))
    for j in range(chunks):
        for dy in range(1, ny):
            tasks.append((4 + 9.0 * (j + 1) + 7 * (dy - 1), functools.partial(hidden_on, 0, j, dy)))
            tasks.append((40 + 7.0 * (j + 1) + 7 * (dy - 1), functools.partial(hidden_on, 1, j, dy)))
        tasks.append((max(30, 4 + 9.0 * (j + 1) + last) + 0.1, functools.partial(layer_two, j)))
        tasks.append((40 + 7.0 * (j + 1) + last + 0.1, functools.partial(layer_three, j)))
    tasks.append((41.0, pick))
    for dz in range(nz):
        for dx in range(nx):
            if dz + dx:
                when = 29.95 if dx == nx - 1 else 5.6 * dz + 6.0 * dx
                tasks.append((when, functools.partial(weight_on, 0, dz, dx)))
            when = 19 + 9.0 * dz + 0.1 * dx if dz else 5.5 + 6.0 * dx
            tasks.append((when, functools.partial(weight_on, 1, dz, dx)))
    for when, color, far in out_blocks(sizes):
        if sum(far.values()) == 0:
            tasks.append((17.0 + color, functools.partial(out_on, color, far, "zx", False, False)))
        else:
            tasks.append((when, functools.partial(out_on, color, far, "yzx", True, True)))

    weight_on(0, 0, 0)
    for color in range(2):
        out_on(color, zero, "y", False, True)
    own_out = [
        local_copy(wo_ref.at[color], out_spot(color, zero, at["c"]), own_sem.at[1 + color])
        for color in range(2)
    ]
    w2_buf[weight_rows(0, 0), :] = w2_ref[...]
    w3_buf[weight_rows(0, 0), :] = w3_ref[...]
    for _, task in sorted(tasks, key=lambda t: t[0]):
        task()

    for _, color, far in out_blocks(sizes):
        arrived(
            out_spot(color, far, 1 - at["c"]),
            q_recv.at[color, far["y"], far["z"], far["x"]], own_sem.at[0],
        )
    for by in range(1, groups):
        source = lax.rem(t_at - by + groups, groups)
        spot = third_ref.at[:, pl.ds(pl.multiple_of(source * width, width), width)]
        arrived(spot, t_recv.at[by], own_sem.at[0])
    for copy in own_out:
        copy.wait()
    for finish in finals:
        finish()
    for copy in started:
        copy.wait_send()


def middle(
    ranges, pot, w_ranges, w_pot, bias_one, w_two, bias_two, w_three, bias_three, w_out
):
    dp, groups = lax.axis_size("dp"), lax.axis_size("tensor")
    nz, nx, ny = factors(dp, groups)
    sizes = {"z": nz, "x": nx, "y": ny}
    states, hands = ranges.shape
    own = states // groups
    width = w_ranges.shape[1]
    rows = w_out.shape[0]
    units = width * groups
    vmem, anywhere = pl.BlockSpec(memory_space=pltpu.VMEM), pl.BlockSpec(memory_space=pl.ANY)
    dma = pltpu.SemaphoreType.DMA
    third, full, picked = pl.pallas_call(
        functools.partial(kernel, sizes),
        out_shape=(
            jax.ShapeDtypeStruct((own, units), jnp.bfloat16),
            jax.ShapeDtypeStruct((dp * groups * 2, rows // 2, hands), jnp.bfloat16),
            jax.ShapeDtypeStruct((own, hands), jnp.bfloat16),
        ),
        in_specs=[anywhere, anywhere] + [vmem] * 8,
        out_specs=(anywhere, anywhere, vmem),
        scratch_shapes=[
            pltpu.VMEM((hands, states), jnp.bfloat16),
            pltpu.VMEM(w_ranges.shape, jnp.bfloat16),
            pltpu.VMEM((states, width), jnp.bfloat16),
            pltpu.VMEM((groups, own, units), jnp.bfloat16),
            pltpu.VMEM((groups, own, units), jnp.bfloat16),
            pltpu.VMEM((groups, own, width), jnp.bfloat16),
            pltpu.VMEM((groups, own, width), jnp.bfloat16),
            pltpu.VMEM((units, width), jnp.bfloat16),
            pltpu.VMEM((units, width), jnp.bfloat16),
            dma((2, nz, nx, 2)),
            dma((2, nz, nx)),
            dma((2, groups, ny, 2)),
            dma((2, groups, ny)),
            dma((2, groups, ny)),
            dma((groups,)),
            dma((groups,)),
            dma((2, ny, nz, nx, 4)),
            dma((2, ny, nz, nx)),
            dma((2, ny, nz, nx)),
            dma((4 + states // math.gcd(states, STEP),)),
        ],
        compiler_params=pltpu.CompilerParams(
            collective_id=0, has_side_effects=True, vmem_limit_bytes=56 * 1024 * 1024
        ),
    )(
        ranges.T, w_ranges, pot[:, None], w_pot[None, :], bias_one[None, :],
        w_two, w_three, w_out.reshape(2, rows // 2, hands), bias_two[None, :], bias_three[None, :],
    )
    return third, full.reshape(units, hands), picked


def local(
    ranges, pot, w_ranges, w_pot, bias_one, w_two, bias_two, w_three, bias_three, w_out, bias_out
):
    own_hidden, out_whole, own_ranges = middle(
        ranges, pot, w_ranges, w_pot, bias_one, w_two, bias_two, w_three, bias_three, w_out
    )
    values = fold_rows(own_hidden, out_whole) + bias_out[None, :]
    weights = own_ranges.astype(jnp.float32)
    error = jnp.sum(weights * values, axis=1) / jnp.sum(weights, axis=1)
    return values - error[:, None]


def solution(mesh):
    in_specs = (
        P("dp", None),
        P("dp"),
        P(None, "tensor"),
        P("tensor"),
        P("tensor"),
        P("dp", "tensor"),
        P("tensor"),
        P("dp", "tensor"),
        P("tensor"),
        P(("dp", "tensor"), None),
        P(),
    )
    out_specs = P(("dp", "tensor"), None)
    return jax.shard_map(local, mesh=mesh, in_specs=in_specs, out_specs=out_specs, check_vma=False)
```

```python
import functools
import math

import jax
import jax.numpy as jnp
from jax import lax
from jax.experimental import pallas as pl
from jax.experimental.pallas import tpu as pltpu
from jax.sharding import PartitionSpec as P

MESH = pl.DeviceIdType.MESH
CORES = 2
STEP = 256
W_ORDERS = (("z", "x"), ("z", "x"))


def relu_round(pre):
    return jnp.maximum(pre, 0.0).astype(jnp.bfloat16)


def fold_rows(left, piece):
    return jnp.dot(left, piece, preferred_element_type=jnp.float32)


def factors(dp, tensor):
    nx = max(f for f in range(1, dp + 1) if dp % f == 0 and f * f <= dp)
    return dp // nx, nx, tensor // CORES


def out_orders():
    return (("z", "y", "x"), ("x", "y", "z"))


def out_blocks(sizes):
    return [
        (color, {"y": dy, "z": dz, "x": dx})
        for color in range(2)
        for dy in range(sizes["y"])
        for dz in range(sizes["z"])
        for dx in range(sizes["x"])
    ]


def onward(order, sizes, far):
    axes = []
    for at, axis in enumerate(order):
        later = order[at + 1 :]
        if far[axis] < sizes[axis] - 1 and all(far[a] == 0 for a in later):
            axes.append(axis)
    return axes


HOLDS = {("oy", 0): 27.9, ("oy", 1): 13.6, ("o", 0): 23.7, ("o", 1): 25.6, ("w", 1): 5.1, "load": 4.0}
RANKS = {"hon": 0, "three": 1, "two": 1, "one": 2, "w": 3, "oy": 4, "o": 5, "pick": 9}


def schedule(sizes, chunks, steps, firsts):
    wire = {"x": 1.0, "y": 1.0, "z": 1.0, "c": 0.078}
    delay = {"x": 1.8, "y": 1.8, "z": 2.6, "c": 1.0}
    w_time, h_time, o_time = 5.6, 7.0, 3.64
    nz, nx, ny = sizes["z"], sizes["x"], sizes["y"]
    plan = {}
    blocks = [(dz, dx) for dz in range(nz) for dx in range(nx)]

    def further(far, axis):
        return tuple(far[a] + (a == axis) for a in "yzx")

    for layer in range(2):
        for dz, dx in blocks:
            far = {"z": dz, "x": dx, "y": 0}
            sends = [
                (a, w_time, ("w", layer) + further(far, a))
                for a in onward(W_ORDERS[layer], sizes, far)
            ]
            first = (("hold", ("w", layer)),)
            needs = (("w", layer, 0, dz, dx),) if dz + dx else first
            plan["w", layer, dz, dx] = (needs, 0.05, sends)
        for j in range(chunks):
            for dy in range(1, ny):
                sends = [("c", h_time, ("p", layer, j, dy))]
                if dy < ny - 1:
                    sends.append(("y", h_time, ("a", layer, j, dy + 1)))
                plan["hon", layer, j, dy] = ((("a", layer, j, dy),), 0.05, sends)
    for i in range(steps):
        sends = []
        for j in range(chunks):
            if firsts[j] == i:
                sends += [("y", h_time, ("a", 0, j, 1)), ("c", h_time, ("p", 0, j, 0))]
        plan["one", i] = ((("hold", "load"),), 2.0, sends)
    for j in range(chunks):
        for layer, name in ((0, "two"), (1, "three")):
            needs = [("p", layer, j, dy) for dy in range(ny)]
            needs += [("done", ("w", layer) + block) for block in blocks]
            needs += [("done", ("hon", layer, j, dy)) for dy in range(1, ny)]
            needs.append(("done", ("two", j) if layer else ("one", firsts[j])))
            sends = [("y", h_time / 2, ("t", j))]
            if layer == 0:
                sends = [("y", h_time, ("a", 1, j, 1)), ("c", h_time, ("p", 1, j, 0))]
            plan[name, j] = (needs, 1.9, sends)
    for color, far in out_blocks(sizes):
        where = tuple(far[a] for a in "yzx")
        sends = [
            (a, o_time, ("o", color) + further(far, a))
            for a in onward(out_orders()[color], sizes, far)
        ]
        mate = ("c", o_time, ("q", color) + where)
        if sum(where):
            plan[("o", color) + where] = ((("o", color) + where,), 0.05, sends + [mate])
        else:
            mine = [send for send in sends if send[0] == "y"] + [mate]
            plan["oy", color] = ((("hold", ("oy", color)),), 0.05, mine)
            rest = [send for send in sends if send[0] != "y"]
            plan[("o", color) + where] = ((("hold", ("o", color)),), 0.05, rest)
    plan["pick",] = (tuple(("done", ("one", i)) for i in range(steps)), 3.0, [])

    free = dict.fromkeys(wire, 0.0)
    there, done, order, now = {}, set(), [], 2.0

    def ready(name):
        at = now
        for need in plan[name][0]:
            if need[0] == "hold":
                at = max(at, HOLDS.get(need[1], 0.0))
            elif need[0] == "done":
                if need[1] not in done:
                    return None
            elif need in there:
                at = max(at, there[need])
            else:
                return None
        return at

    def rank(name):
        tail = name[1:] if name[0] != "o" else (name[1], name[3], name[2], name[4])
        return (RANKS[name[0]], name[1] if name[0] == "w" else 0) + tuple(tail)

    todo = list(plan)
    while todo:
        open_now = [(ready(name), rank(name), name) for name in todo]
        open_now = [entry for entry in open_now if entry[0] is not None]
        soonest = min(entry[0] for entry in open_now)
        at, _, name = min(
            (entry for entry in open_now if entry[0] <= soonest + 1e-9), key=lambda entry: entry[1]
        )
        todo.remove(name)
        now = at + plan[name][1]
        done.add(name)
        order.append(name)
        for axis, cost, key in plan[name][2]:
            free[axis] = max(free[axis], now) + cost * wire[axis]
            there[key] = free[axis] + delay[axis]
    return order


def kernel(
    sizes, ranges_ref, wr_ref, pot_ref, wp_ref, b1_ref, w2_ref, w3_ref, wo_ref, b2_ref, b3_ref,
    third_ref, full_ref, picked_ref,
    ranges_buf, wr_buf, stage1, act2, act3, stage2, stage3, w2_buf, w3_buf,
    w_send, w_recv, a_send, a_recv, p_recv, t_send, t_recv, o_send, o_recv, q_recv, own_sem,
):
    nz, nx, ny = sizes["z"], sizes["x"], sizes["y"]
    groups = ny * CORES
    dp_at, t_at = lax.axis_index("dp"), lax.axis_index("tensor")
    at = {
        "z": lax.div(dp_at, nx), "x": lax.rem(dp_at, nx),
        "y": lax.div(t_at, CORES), "c": lax.rem(t_at, CORES),
    }

    def shifted(axis, by):
        return lax.rem(at[axis] + by + sizes[axis], sizes[axis])

    def dev(z=None, x=None, y=None, c=None):
        z = at["z"] if z is None else z
        x = at["x"] if x is None else x
        y = at["y"] if y is None else y
        c = at["c"] if c is None else c
        return {"dp": z * nx + x, "tensor": y * CORES + c}

    nexts = {axis: dev(**{axis: shifted(axis, 1)}) for axis in ("z", "x", "y")}
    partner = dev(c=1 - at["c"])

    states = ranges_ref.shape[1]
    steps = states // math.gcd(states, STEP)
    tall = states // steps
    loads = [
        pltpu.make_async_copy(
            ranges_ref.at[:, pl.ds(i * tall, tall)], ranges_buf.at[:, pl.ds(i * tall, tall)],
            own_sem.at[3 + i],
        )
        for i in range(steps)
    ]
    load_wr = pltpu.make_async_copy(wr_ref, wr_buf, own_sem.at[3 + steps])
    load_wr.start()
    for load in loads:
        load.start()

    barrier = pltpu.get_barrier_semaphore()
    greeted = 0
    for axis in ("z", "x"):
        for by in {1 % sizes[axis], sizes[axis] - 1} - {0}:
            pl.semaphore_signal(
                barrier, inc=1, device_id=dev(**{axis: shifted(axis, by)}), device_id_type=MESH
            )
            greeted += 1
    for by in range(1, groups):
        pl.semaphore_signal(
            barrier, inc=1,
            device_id={"dp": dp_at, "tensor": lax.rem(t_at + by, groups)}, device_id_type=MESH,
        )
        greeted += 1
    pl.semaphore_wait(barrier, greeted)

    started = []

    def send(src, dst, s_sem, r_sem, to):
        copy = pltpu.make_async_remote_copy(
            src_ref=src, dst_ref=dst, send_sem=s_sem, recv_sem=r_sem,
            device_id=to, device_id_type=MESH,
        )
        copy.start()
        started.append(copy)

    def arrived(ref, sem, spare):
        pltpu.make_async_remote_copy(
            src_ref=ref, dst_ref=ref, send_sem=spare, recv_sem=sem,
            device_id=partner, device_id_type=MESH,
        ).wait_recv()

    def local_copy(src, dst, sem):
        copy = pltpu.make_async_copy(src, dst, sem)
        copy.start()
        return copy

    chunks, own, width = stage2.shape
    firsts = [((j + 1) * own - 1) // tall for j in range(chunks)]
    depth = w2_ref.shape[0]
    sizes_w = {"z": nz, "x": nx}

    def columns(dy, core):
        piece = shifted("y", -dy) * CORES + core
        return pl.ds(pl.multiple_of(piece * width, width), width)

    def hidden_send(layer, j, dy, src):
        act = (act2, act3)[layer]
        spot = act.at[j, :, columns(dy, at["c"])]
        src = spot if src is None else src
        if dy < ny - 1:
            send(src, spot, a_send.at[layer, j, dy, 0], a_recv.at[layer, j, dy + 1], nexts["y"])
        send(src, spot, a_send.at[layer, j, dy, 1], p_recv.at[layer, j, dy], partner)

    def hidden_on(layer, j, dy):
        act = (act2, act3)[layer]
        arrived(act.at[j, :, columns(dy, at["c"])], a_recv.at[layer, j, dy], own_sem.at[0])
        hidden_send(layer, j, dy, None)

    def weight_rows(dz, dx):
        row = shifted("z", -dz) * nx + shifted("x", -dx)
        return pl.ds(pl.multiple_of(row * depth, depth), depth)

    def weight_on(layer, dz, dx):
        buf, ref = ((w2_buf, w2_ref), (w3_buf, w3_ref))[layer]
        spot = buf.at[weight_rows(dz, dx), :]
        src = spot
        if dz == 0 and dx == 0:
            src = ref
        else:
            arrived(spot, w_recv.at[layer, dz, dx], own_sem.at[0])
        for axis in onward(W_ORDERS[layer], sizes_w, {"z": dz, "x": dx}):
            to_z, to_x = (dz + 1, dx) if axis == "z" else (dz, dx + 1)
            which = 0 if axis == "z" else 1
            send(src, spot, w_send.at[layer, dz, dx, which], w_recv.at[layer, to_z, to_x], nexts[axis])

    def out_spot(color, far, core):
        row = shifted("z", -far["z"]) * nx + shifted("x", -far["x"])
        return full_ref.at[(row * groups + shifted("y", -far["y"]) * CORES + core) * 2 + color]

    def out_on(color, far, axes, wait, mate):
        order = out_orders()[color]
        spot = out_spot(color, far, at["c"])
        where = (color, far["y"], far["z"], far["x"])
        src = wo_ref.at[color] if sum(far.values()) == 0 else spot
        if wait and sum(far.values()):
            arrived(spot, o_recv.at[where], own_sem.at[0])
        for axis in onward(order, sizes, far):
            if axis not in axes:
                continue
            to = dict(far)
            to[axis] += 1
            send(
                src, spot, o_send.at[where + ("yzx".index(axis),)],
                o_recv.at[color, to["y"], to["z"], to["x"]], nexts[axis],
            )
        if mate:
            send(src, spot, o_send.at[where + (3,)], q_recv.at[where], partner)

    def compute(layer, j):
        act, buf, bias = ((act2, w2_buf, b2_ref), (act3, w3_buf, b3_ref))[layer]
        return relu_round(fold_rows(act[j], buf[...]) + bias[...])

    def pieces_here(layer, j):
        act = (act2, act3)[layer]
        for dy in range(ny):
            arrived(act.at[j, :, columns(dy, 1 - at["c"])], p_recv.at[layer, j, dy], own_sem.at[0])

    def layer_two(j):
        pieces_here(0, j)
        hidden = compute(0, j)
        stage2[j] = hidden
        act3[j, :, columns(0, at["c"])] = hidden
        hidden_send(1, j, 0, stage2.at[j])

    def layer_one(i):
        if i == 0:
            load_wr.wait()
        loads[i].wait()
        at_rows = pl.ds(i * tall, tall)
        pre = lax.dot_general(
            ranges_buf[:, at_rows], wr_buf[...], (((0,), (0,)), ((), ())),
            preferred_element_type=jnp.float32,
        )
        stage1[at_rows, :] = relu_round(pre + pot_ref[at_rows, :] * wp_ref[...] + b1_ref[...])
        for j in range(chunks):
            if firsts[j] == i:
                rows = pl.ds(j * own, own)
                act2[j, :, columns(0, at["c"])] = stage1[rows, :]
                hidden_send(0, j, 0, stage1.at[rows, :])

    def pick():
        wanted = lax.broadcasted_iota(jnp.int32, (own, states), 0) + t_at * own
        found = lax.broadcasted_iota(jnp.int32, (own, states), 1) == wanted
        picked_ref[...] = lax.dot_general(
            jnp.where(found, 1.0, 0.0).astype(jnp.bfloat16), ranges_buf[...],
            (((1,), (1,)), ((), ())), preferred_element_type=jnp.float32,
        ).astype(jnp.bfloat16)

    finals = []

    def layer_three(j):
        pieces_here(1, j)
        stage3[j] = compute(1, j)
        mine = third_ref.at[:, pl.ds(pl.multiple_of(t_at * width, width), width)]
        far = lax.rem(j - t_at + groups, groups)

        def away():
            return pltpu.make_async_remote_copy(
                src_ref=stage3.at[j], dst_ref=mine, send_sem=t_send.at[j], recv_sem=t_recv.at[far],
                device_id={"dp": dp_at, "tensor": jnp.int32(j)}, device_id_type=MESH,
            )

        def here():
            return pltpu.make_async_copy(stage3.at[j], mine, t_send.at[j])

        @pl.when(t_at != j)
        def _():
            away().start()

        @pl.when(t_at == j)
        def _():
            here().start()

        def finish():
            @pl.when(t_at != j)
            def _():
                away().wait_send()

            @pl.when(t_at == j)
            def _():
                here().wait()

        finals.append(finish)

    zero = {"y": 0, "z": 0, "x": 0}
    own_out = [
        local_copy(wo_ref.at[color], out_spot(color, zero, at["c"]), own_sem.at[1 + color])
        for color in range(2)
    ]
    w2_buf[weight_rows(0, 0), :] = w2_ref[...]
    w3_buf[weight_rows(0, 0), :] = w3_ref[...]
    for name in schedule(sizes, chunks, steps, firsts):
        kind = name[0]
        if kind == "w":
            weight_on(*name[1:])
        elif kind == "hon":
            hidden_on(*name[1:])
        elif kind == "one":
            layer_one(name[1])
        elif kind == "two":
            layer_two(name[1])
        elif kind == "three":
            layer_three(name[1])
        elif kind == "pick":
            pick()
        elif kind == "oy":
            out_on(name[1], zero, "y", False, True)
        else:
            far = dict(zip("yzx", name[2:]))
            mine = sum(name[2:]) == 0
            out_on(name[1], far, "zx" if mine else "yzx", not mine, not mine)

    for color, far in out_blocks(sizes):
        arrived(
            out_spot(color, far, 1 - at["c"]),
            q_recv.at[color, far["y"], far["z"], far["x"]], own_sem.at[0],
        )
    for by in range(1, groups):
        source = lax.rem(t_at - by + groups, groups)
        spot = third_ref.at[:, pl.ds(pl.multiple_of(source * width, width), width)]
        arrived(spot, t_recv.at[by], own_sem.at[0])
    for copy in own_out:
        copy.wait()
    for finish in finals:
        finish()
    for copy in started:
        copy.wait_send()


def middle(
    ranges, pot, w_ranges, w_pot, bias_one, w_two, bias_two, w_three, bias_three, w_out
):
    dp, groups = lax.axis_size("dp"), lax.axis_size("tensor")
    nz, nx, ny = factors(dp, groups)
    sizes = {"z": nz, "x": nx, "y": ny}
    states, hands = ranges.shape
    own = states // groups
    width = w_ranges.shape[1]
    rows = w_out.shape[0]
    units = width * groups
    vmem, anywhere = pl.BlockSpec(memory_space=pltpu.VMEM), pl.BlockSpec(memory_space=pl.ANY)
    dma = pltpu.SemaphoreType.DMA
    third, full, picked = pl.pallas_call(
        functools.partial(kernel, sizes),
        out_shape=(
            jax.ShapeDtypeStruct((own, units), jnp.bfloat16),
            jax.ShapeDtypeStruct((dp * groups * 2, rows // 2, hands), jnp.bfloat16),
            jax.ShapeDtypeStruct((own, hands), jnp.bfloat16),
        ),
        in_specs=[anywhere, anywhere] + [vmem] * 8,
        out_specs=(anywhere, anywhere, vmem),
        scratch_shapes=[
            pltpu.VMEM((hands, states), jnp.bfloat16),
            pltpu.VMEM(w_ranges.shape, jnp.bfloat16),
            pltpu.VMEM((states, width), jnp.bfloat16),
            pltpu.VMEM((groups, own, units), jnp.bfloat16),
            pltpu.VMEM((groups, own, units), jnp.bfloat16),
            pltpu.VMEM((groups, own, width), jnp.bfloat16),
            pltpu.VMEM((groups, own, width), jnp.bfloat16),
            pltpu.VMEM((units, width), jnp.bfloat16),
            pltpu.VMEM((units, width), jnp.bfloat16),
            dma((2, nz, nx, 2)),
            dma((2, nz, nx)),
            dma((2, groups, ny, 2)),
            dma((2, groups, ny)),
            dma((2, groups, ny)),
            dma((groups,)),
            dma((groups,)),
            dma((2, ny, nz, nx, 4)),
            dma((2, ny, nz, nx)),
            dma((2, ny, nz, nx)),
            dma((4 + states // math.gcd(states, STEP),)),
        ],
        compiler_params=pltpu.CompilerParams(
            collective_id=0, has_side_effects=True, vmem_limit_bytes=56 * 1024 * 1024
        ),
    )(
        ranges.T, w_ranges, pot[:, None], w_pot[None, :], bias_one[None, :],
        w_two, w_three, w_out.reshape(2, rows // 2, hands), bias_two[None, :], bias_three[None, :],
    )
    return third, full.reshape(units, hands), picked


def local(
    ranges, pot, w_ranges, w_pot, bias_one, w_two, bias_two, w_three, bias_three, w_out, bias_out
):
    own_hidden, out_whole, own_ranges = middle(
        ranges, pot, w_ranges, w_pot, bias_one, w_two, bias_two, w_three, bias_three, w_out
    )
    values = fold_rows(own_hidden, out_whole) + bias_out[None, :]
    weights = own_ranges.astype(jnp.float32)
    error = jnp.sum(weights * values, axis=1) / jnp.sum(weights, axis=1)
    return values - error[:, None]


def solution(mesh):
    in_specs = (
        P("dp", None),
        P("dp"),
        P(None, "tensor"),
        P("tensor"),
        P("tensor"),
        P("dp", "tensor"),
        P("tensor"),
        P("dp", "tensor"),
        P("tensor"),
        P(("dp", "tensor"), None),
        P(),
    )
    out_specs = P(("dp", "tensor"), None)
    return jax.shard_map(local, mesh=mesh, in_specs=in_specs, out_specs=out_specs, check_vma=False)
```
